32 devices in a mesh: grp: 4 (over y, core), rep: 8 (over z, x).
Axes of the slice: x: 2, y: 2, z: 4, core: 2. Of those that a mesh axis runs over, the one named last changes fastest.
Arguments:
- coefficients: bfloat16 [4096, 2048], P(('grp', 'rep')), may hold values from -100 to 100
- truncation: int32 [16], replicated, may hold values from 16 to 64
- neighbours: int32 [50, 4096], P(None, ('grp', 'rep')), may hold values from 0 to 4095, as said below
- initial: float32 [32, 4096], P(None, ('grp', 'rep')), may hold values from -6 to 6
Outputs:
- alignment: float32 [2, 50, 4096], P(None, None, ('grp', 'rep'))
- vectors: float32 [32, 4096], P(None, ('grp', 'rep'))
The draws below stay inside these ranges and needn't reach their ends.
Inputs may be any that keep to these rules, and one draw needn't show every extreme that they name: `neighbours`: every neighbour of a particle is another particle of the same block of 1024 particles that holds it (the particles of one group of 8 devices along rep). For each device, the neighbour slots of its 128 particles that name particles of one other device number at most 64; every device has, in every draw, one other device that its slots name exactly 64 times.
All inputs are finite; a program needn't handle non-finite values.
Results may differ from the reference program's by a relative error of at most 0.0003.
Values may be sent and summed in bfloat16 or wider, within the bound.
A program may use at most 128 MiB of HBM per device.

```python
import math
import jax
import jax.numpy as jnp
from jax import lax

ANG = 64
RAD = 16
ANGLES = 256
NB = 50
VEC = 16
ITERS = 3
P_DEV = 128
CAP = 64
CW = 2048
NPART = 4096
N_REP = 8


def draw_coefficients(key, part):
    scale_key, noise_key = jax.random.split(key, 2)
    row_scale = jnp.exp(jax.random.uniform(scale_key, (NPART, 1), jnp.float32, 0.0, math.log(10.0)))
    noise = jnp.clip(jax.random.normal(noise_key, (NPART, CW), jnp.float32), -6.0, 6.0)
    return (row_scale * noise).astype(jnp.bfloat16)


def draw_neighbours(key, part):
    devices = NPART // P_DEV
    slots = NB * P_DEV
    peers = N_REP - 1
    count_key, complete_random_key, order_key, near_key, far_key = jax.random.split(key, 5)
    counts = jax.random.randint(count_key, (devices, peers), CAP // 4, CAP // 2 + 1)
    chosen = jax.random.randint(complete_random_key, (devices, 1), 0, peers)
    counts = jnp.where(jnp.arange(peers, dtype=jnp.int32)[None, :] == chosen, CAP, counts).astype(jnp.int32)
    bounds = jnp.cumsum(counts, axis=1).astype(jnp.int32)
    order_keys = jax.random.split(order_key, devices)
    ranks = jax.vmap(lambda single: jax.random.permutation(single, slots))(order_keys).astype(jnp.int32)
    offsets = jax.vmap(lambda edges, values: jnp.searchsorted(edges, values, side='right'))(bounds, ranks).astype(jnp.int32)
    remote = offsets < peers
    device_ids = jnp.arange(devices, dtype=jnp.int32)[:, None]
    own_rep = device_ids % N_REP
    group_start = device_ids // N_REP * (N_REP * P_DEV)
    peer_rep = (own_rep + 1 + offsets) % N_REP
    particle = jnp.arange(slots, dtype=jnp.int32)[None, :] % P_DEV
    near = (particle + jax.random.randint(near_key, (devices, slots), 1, P_DEV)) % P_DEV
    far = jax.random.randint(far_key, (devices, slots), 0, P_DEV)
    owner_rep = jnp.where(remote, peer_rep, own_rep)
    within = jnp.where(remote, far, near)
    global_ids = group_start + owner_rep * P_DEV + within
    return global_ids.reshape(devices, NB, P_DEV).transpose(1, 0, 2).reshape(NB, NPART).astype(jnp.int32)


def set_ends(drawn, rng, low, top_value):
    longest = drawn.shape.index(max(drawn.shape))
    spots = []
    for shift in (0, 1):
        where = [jax.random.randint(jax.random.fold_in(rng, axis), (), 0, length) for axis, length in enumerate(drawn.shape)]
        where[longest] = (where[longest] + shift) % drawn.shape[longest]
        spots.append(tuple(where))
    return drawn.at[spots[0]].set(low).at[spots[1]].set(top_value)


def shard_levels(stream_key, dims, pieces, low, largest):
    loudness = 1.0
    for dim, parts in pieces:
        steps = jax.random.uniform(jax.random.fold_in(jax.random.fold_in(stream_key, 6), dim), (parts,), jnp.float32, low / len(pieces), largest / len(pieces))
        loudness = loudness * jnp.repeat(jnp.exp(steps), dims[dim] // parts).reshape((-1,) + (1,) * (len(dims) - 1 - dim))
    return loudness


def bell_draw(rng, dims, deviation, most, cuts=(), kind=jnp.bfloat16):
    entries = jax.random.normal(rng, dims, jnp.float32) * deviation
    if len(cuts) > 0:
        entries = shard_levels(rng, dims, cuts, -0.22, 0.18) * entries
    return jnp.clip(entries, min=-most, max=most).astype(kind)


def setup_inputs(seed: int = 0) -> dict:
    seeds = jax.random.split(jax.random.key(seed), 5)
    coefficients = draw_coefficients(jax.random.fold_in(seeds[4], 71), 0)
    truncation = set_ends(jax.random.randint(seeds[1], (RAD,), ANG // 4, ANG + 1), jax.random.fold_in(seeds[1], 1), ANG // 4, ANG).astype(jnp.int32)
    neighbours = draw_neighbours(jax.random.fold_in(seeds[4], 71), 0)
    initial = bell_draw(seeds[3], (2 * VEC, NPART), 1.0, 6.0, ((1, 32),), jnp.float32)
    return {"coefficients": coefficients, "truncation": truncation, "neighbours": neighbours, "initial": initial}


epsilon = 1e-06

def rotation_angle_grid(angular, samples):
    frequency = jnp.arange(angular, dtype=jnp.float32)
    sample_angle = jnp.arange(samples, dtype=jnp.float32) * (2.0 * math.pi / samples)
    phases = frequency[:, None] * sample_angle[None, :]
    transform = jnp.concatenate([jnp.cos(phases), -jnp.sin(phases)], axis=0)
    return (transform, jnp.cos(sample_angle), jnp.sin(sample_angle))

def kept_mask(truncation):
    levels = jnp.arange(ANG, dtype=jnp.int32)
    return (levels[None, :] < truncation[:, None]).astype(jnp.float32)

def pair_moments(own_rows, other_rows, weights, transform, cosine_row, sine_row):
    row_count = own_rows.shape[0]
    local_complete = own_rows.astype(jnp.float32).reshape(row_count, 2, RAD, ANG) * weights
    partner_complete = other_rows.astype(jnp.float32).reshape(NB, row_count, 2, RAD, ANG)
    maximum_frequency = lax.Precision.HIGHEST
    real_fourier_coeffs = jnp.einsum('fwh,rfwh->rfh', local_complete[:, 0], partner_complete[:, :, 0], precision=maximum_frequency)
    real_fourier_coeffs = real_fourier_coeffs + jnp.einsum('fwh,rfwh->rfh', local_complete[:, 1], partner_complete[:, :, 1], precision=maximum_frequency)
    imaginary_fourier_coeffs = jnp.einsum('fwh,rfwh->rfh', local_complete[:, 1], partner_complete[:, :, 0], precision=maximum_frequency)
    imaginary_fourier_coeffs = imaginary_fourier_coeffs - jnp.einsum('fwh,rfwh->rfh', local_complete[:, 0], partner_complete[:, :, 1], precision=maximum_frequency)
    spectrum = jnp.concatenate([real_fourier_coeffs, imaginary_fourier_coeffs], axis=2)
    correlation = jnp.einsum('nbk,km->nbm', spectrum, transform, precision=maximum_frequency)
    squared = correlation * correlation
    energy = jnp.mean(squared, axis=2)
    moment_real = jnp.mean(squared * cosine_row, axis=2)
    moment_imaginary = jnp.mean(squared * sine_row, axis=2)
    return (energy, moment_real, moment_imaginary)

def lower_inverse(lower):
    matrix_order = lower.shape[0]
    identity = jnp.eye(matrix_order, dtype=lower.dtype)
    inverse_rows = []
    for target in range(matrix_order):
        running = identity[target]
        for source in range(target):
            running = running - lower[target, source] * inverse_rows[source]
        inverse_rows.append(running / lower[target, target])
    return jnp.stack(inverse_rows)

def reference(coefficients, truncation, neighbours, initial):
    maximum_frequency = lax.Precision.HIGHEST
    weights = kept_mask(truncation)
    transform, cosine_row, sine_row = rotation_angle_grid(ANG, ANGLES)
    particle_total = coefficients.shape[0]
    block_width = math.gcd(particle_total, 128)
    blocks = particle_total // block_width
    own_blocks = coefficients.reshape(blocks, block_width, coefficients.shape[1])
    index_blocks = neighbours.reshape(NB, blocks, block_width).transpose(1, 0, 2)

    def one_block(operands):
        own_rows, indices = operands
        other_rows = jnp.take(coefficients, indices.reshape(-1), axis=0)
        return pair_moments(own_rows, other_rows, weights, transform, cosine_row, sine_row)
    energy, moment_real, moment_imaginary = lax.map(one_block, (own_blocks, index_blocks))
    energy = energy.transpose(1, 0, 2).reshape(NB, particle_total)
    moment_real = moment_real.transpose(1, 0, 2).reshape(NB, particle_total)
    moment_imaginary = moment_imaginary.transpose(1, 0, 2).reshape(NB, particle_total)
    alignment = jnp.stack([moment_real / (energy + epsilon), moment_imaginary / (energy + epsilon)])
    degree = epsilon + jnp.sum(energy, axis=0)
    current = initial
    vector_count = initial.shape[0] // 2
    for iteration in range(ITERS):
        picked = jnp.take(current, neighbours.reshape(-1), axis=1).reshape(current.shape[0], NB, particle_total)
        real_part = picked[:vector_count]
        imag_part = picked[vector_count:]
        image_real = jnp.sum(moment_real * real_part - moment_imaginary * imag_part, axis=1) / degree
        image_imag = jnp.sum(moment_real * imag_part + moment_imaginary * real_part, axis=1) / degree
        gram_matrix = (jnp.dot(image_real, image_real.T, precision=maximum_frequency) + jnp.dot(image_imag, image_imag.T, precision=maximum_frequency)) / particle_total
        inverse = lower_inverse(jnp.linalg.cholesky(gram_matrix))
        current = jnp.concatenate([jnp.dot(inverse, image_real, precision=maximum_frequency), jnp.dot(inverse, image_imag, precision=maximum_frequency)], axis=0)
    return (alignment, current)
```

```python
import functools
import math

import jax
import jax.numpy as jnp
from jax import lax
from jax.experimental import pallas as pl
from jax.experimental.pallas import tpu as pltpu
from jax.sharding import PartitionSpec as P

ANG = 64
RAD = 16
ITERS = 3
EPS = 1e-06
VMEM = pl.BlockSpec(memory_space=pltpu.VMEM)


def moments_kernel(own_ref, all_ref, slots_ref, slots_t_ref, align_ref, oper_ref, degree_ref, ar_ref, ai_ref):
    blocks, _, _, wide = all_ref.shape
    own = own_ref.shape[2] // 2
    slots = slots_ref.shape[0]
    half = wide // 2

    degree_ref[...] = jnp.full(degree_ref.shape, EPS, jnp.float32)

    def tile(step, _):
        block = step // 2
        part = step % 2
        energy = moment_re = moment_im = before_re = before_im = None
        for k in range(ANG):
            partner = all_ref[block, k].T
            partner = jnp.where(part == 0, partner[:half], partner[half:])
            spectrum = jnp.dot(partner, own_ref[k], preferred_element_type=jnp.float32)
            re, im = spectrum[:, :own], spectrum[:, own:]
            if k == 0:
                energy = 2.0 * (re * re)
                before_re = 2.0 * re
                continue
            energy = energy + (re * re + im * im)
            if k == 1:
                moment_re = before_re * re
                moment_im = -(before_re * im)
            else:
                moment_re = moment_re + (before_re * re + before_im * im)
                moment_im = moment_im + (before_im * re - before_re * im)
            before_re, before_im = re, im
        energy, moment_re, moment_im = 0.5 * energy, 0.5 * moment_re, 0.5 * moment_im
        first = pl.multiple_of(step * half, half)
        rows = pl.ds(first, half)
        name = lax.broadcasted_iota(jnp.int32, (half, own), 0) + first
        count = jnp.zeros((half, own), jnp.float32)
        for n in range(slots):
            count = count + jnp.where(slots_ref[n : n + 1, :] == name, 1.0, 0.0)
        oper_ref[rows, :own] = count * moment_re
        oper_ref[rows, own:] = count * moment_im
        degree_ref[...] += jnp.sum(count * energy, axis=0, keepdims=True)
        scale = 1.0 / (energy + EPS)
        ar_ref[rows, :] = moment_re * scale
        ai_ref[rows, :] = moment_im * scale
        return 0

    lax.fori_loop(0, 2 * blocks, tile, 0)

    names = slots_t_ref[...]
    lane = names % wide
    owner = names // wide

    def pick(block, found):
        rows = pl.ds(pl.multiple_of(block * wide, wide), wide)
        here = owner == block
        got_re = jnp.take_along_axis(ar_ref[rows, :].T, lane, axis=1, mode="promise_in_bounds")
        got_im = jnp.take_along_axis(ai_ref[rows, :].T, lane, axis=1, mode="promise_in_bounds")
        return (jnp.where(here, got_re, found[0]), jnp.where(here, got_im, found[1]))

    zero = jnp.zeros(names.shape, jnp.float32)
    found = lax.fori_loop(0, blocks, pick, (zero, zero))
    align_ref[0] = found[0].T[:slots]
    align_ref[1] = found[1].T[:slots]


def whiten_kernel(gram_ref, image_ref, out_ref):
    order = gram_ref.shape[0]
    lanes = image_ref.shape[1]
    gram = gram_ref[...]
    right = jnp.concatenate([image_ref[:order], image_ref[order:]], axis=1)
    row = lax.broadcasted_iota(jnp.int32, (order, 1), 0)
    for p in range(order):
        pivot = gram[p : p + 1, p : p + 1]
        factor = jnp.where(row > p, gram[:, p : p + 1] / pivot, 0.0)
        scale = jnp.where(row == p, lax.rsqrt(pivot), 1.0)
        new_right = (right - factor * right[p : p + 1]) * scale
        gram = gram - factor * gram[p : p + 1]
        right = new_right
    out_ref[:order] = right[:, :lanes]
    out_ref[order:] = right[:, lanes:]


def shards(coefficients, truncation, neighbours, initial):
    highest = lax.Precision.HIGHEST
    groups = lax.axis_size("grp")
    replicas = lax.axis_size("rep")
    particles = coefficients.shape[0]
    slots = neighbours.shape[0]
    total = particles * groups * replicas
    in_group = neighbours - lax.axis_index("grp") * (replicas * particles)
    padded = jnp.pad(in_group.T, ((0, 0), (0, 128 - slots)))

    mine = coefficients.reshape(particles, 2 * RAD, ANG).transpose(2, 1, 0)
    everyone = lax.all_gather(mine, "rep", axis=0)
    kept = jnp.arange(ANG, dtype=jnp.int32)[:, None] < truncation[None, :]
    kept = jnp.concatenate([kept, kept], axis=1)[:, :, None]
    turned = jnp.concatenate([mine[:, RAD:], -mine[:, :RAD]], axis=1)
    own = jnp.concatenate([mine, turned], axis=2)
    own = jnp.where(kept, own, jnp.zeros_like(own))

    group = replicas * particles
    alignment, operator, degree = pl.pallas_call(
        moments_kernel,
        out_shape=[
            jax.ShapeDtypeStruct((2, slots, particles), jnp.float32),
            jax.ShapeDtypeStruct((group, 2 * particles), jnp.float32),
            jax.ShapeDtypeStruct((1, particles), jnp.float32),
        ],
        in_specs=[VMEM] * 4,
        out_specs=[VMEM] * 3,
        scratch_shapes=[pltpu.VMEM((group, particles), jnp.float32)] * 2,
        name="moments",
    )(own, everyone, in_group, padded)

    count = initial.shape[0] // 2
    current = initial
    for _ in range(ITERS):
        whole = lax.all_gather(current, "rep", axis=1, tiled=True)
        product = jnp.dot(whole, operator, precision=highest)
        image_re = product[:count, :particles] - product[count:, particles:]
        image_im = product[count:, :particles] + product[:count, particles:]
        current = jnp.concatenate([image_re, image_im], axis=0) / degree
    image_re, image_im = current[:count], current[count:]
    gram = lax.psum(
        (jnp.dot(image_re, image_re.T, precision=highest) + jnp.dot(image_im, image_im.T, precision=highest)) / total,
        ("grp", "rep"),
    )
    vectors = pl.pallas_call(
        whiten_kernel,
        out_shape=jax.ShapeDtypeStruct(initial.shape, jnp.float32),
        in_specs=[VMEM] * 2,
        out_specs=VMEM,
        name="whiten",
    )(gram, current)
    return alignment, vectors


def solution(mesh):
    in_specs = (P(("grp", "rep"), None), P(), P(None, ("grp", "rep")), P(None, ("grp", "rep")))
    out_specs = (P(None, None, ("grp", "rep")), P(None, ("grp", "rep")))
    return jax.shard_map(shards, mesh=mesh, in_specs=in_specs, out_specs=out_specs, check_vma=False)
```

```python
import functools
import math

import jax
import jax.numpy as jnp
from jax import lax
from jax.experimental import pallas as pl
from jax.experimental.pallas import tpu as pltpu
from jax.sharding import PartitionSpec as P

ANG = 64
RAD = 16
ITERS = 3
EPS = 1e-06
MESH = pl.DeviceIdType.MESH
VMEM = pl.BlockSpec(memory_space=pltpu.VMEM)


def moments_kernel(own_ref, all_ref, slots_ref, slots_t_ref, align_ref, oper_ref, degree_ref, ar_ref, ai_ref):
    blocks, _, _, wide = all_ref.shape
    own = own_ref.shape[2] // 2
    slots = slots_ref.shape[0]
    half = wide // 2

    degree_ref[...] = jnp.full(degree_ref.shape, EPS, jnp.float32)

    def tile(step, _):
        block = step // 2
        part = step % 2
        energy = moment_re = moment_im = before_re = before_im = None
        for k in range(ANG):
            partner = all_ref[block, k].T
            partner = jnp.where(part == 0, partner[:half], partner[half:])
            spectrum = jnp.dot(partner, own_ref[k], preferred_element_type=jnp.float32)
            re, im = spectrum[:, :own], spectrum[:, own:]
            if k == 0:
                energy = 2.0 * (re * re)
                before_re = 2.0 * re
                continue
            energy = energy + (re * re + im * im)
            if k == 1:
                moment_re = before_re * re
                moment_im = -(before_re * im)
            else:
                moment_re = moment_re + (before_re * re + before_im * im)
                moment_im = moment_im + (before_im * re - before_re * im)
            before_re, before_im = re, im
        energy, moment_re, moment_im = 0.5 * energy, 0.5 * moment_re, 0.5 * moment_im
        first = pl.multiple_of(step * half, half)
        rows = pl.ds(first, half)
        name = lax.broadcasted_iota(jnp.int32, (half, own), 0) + first
        count = jnp.zeros((half, own), jnp.float32)
        for n in range(slots):
            count = count + jnp.where(slots_ref[n : n + 1, :] == name, 1.0, 0.0)
        oper_ref[rows, :own] = count * moment_re
        oper_ref[rows, own:] = count * moment_im
        degree_ref[...] += jnp.sum(count * energy, axis=0, keepdims=True)
        scale = 1.0 / (energy + EPS)
        ar_ref[rows, :] = moment_re * scale
        ai_ref[rows, :] = moment_im * scale
        return 0

    lax.fori_loop(0, 2 * blocks, tile, 0)

    names = slots_t_ref[...]
    lane = names % wide
    owner = names // wide

    def pick(block, found):
        rows = pl.ds(pl.multiple_of(block * wide, wide), wide)
        here = owner == block
        got_re = jnp.take_along_axis(ar_ref[rows, :].T, lane, axis=1, mode="promise_in_bounds")
        got_im = jnp.take_along_axis(ai_ref[rows, :].T, lane, axis=1, mode="promise_in_bounds")
        return (jnp.where(here, got_re, found[0]), jnp.where(here, got_im, found[1]))

    zero = jnp.zeros(names.shape, jnp.float32)
    found = lax.fori_loop(0, blocks, pick, (zero, zero))
    align_ref[0] = found[0].T[:slots]
    align_ref[1] = found[1].T[:slots]


def diffuse_kernel(oper_ref, degree_ref, initial_ref, out_ref, land, image, part_gram, land_rep, land_grp, *sems):
    send, recv, send_rep, recv_rep, send_grp, recv_grp = sems
    groups, replicas = lax.axis_size("grp"), lax.axis_size("rep")
    grp, rep = lax.axis_index("grp"), lax.axis_index("rep")
    rows, particles = initial_ref.shape
    order = rows // 2
    highest = lax.Precision.HIGHEST

    def on_rep(step):
        return (grp, lax.rem(rep + step, replicas))

    def on_grp(step):
        return (lax.rem(grp + step, groups), rep)

    barrier = pltpu.get_barrier_semaphore()
    for step in range(1, replicas):
        pl.semaphore_signal(barrier, inc=1, device_id=on_rep(step), device_id_type=MESH)
    for step in range(1, groups):
        pl.semaphore_signal(barrier, inc=1, device_id=on_grp(step), device_id_type=MESH)
    pl.semaphore_wait(barrier, replicas + groups - 2)

    def spread(src, dst, out_sems, in_sems, peer, count):
        copies = []
        for step in range(1, count):
            copy = pltpu.make_async_remote_copy(
                src_ref=src,
                dst_ref=dst,
                send_sem=out_sems.at[step],
                recv_sem=in_sems.at[step],
                device_id=peer(step),
                device_id_type=MESH,
            )
            copy.start()
            copies.append(copy)
        return copies

    started = []
    for turn in range(ITERS):
        src = initial_ref if turn == 0 else image.at[turn - 1]
        copies = spread(src, land.at[turn, rep], send.at[turn], recv.at[turn], on_rep, replicas)
        land[turn, pl.ds(rep, 1)] = src[...][None]
        started += copies
        for copy in copies:
            copy.wait_recv()
        whole = jnp.concatenate([land[turn, r] for r in range(replicas)], axis=1)
        product = jnp.dot(whole, oper_ref[...], precision=highest, preferred_element_type=jnp.float32)
        image_re = (product[:order, :particles] - product[order:, particles:]) / degree_ref[...]
        image_im = (product[order:, :particles] + product[:order, particles:]) / degree_ref[...]
        if turn < ITERS - 1:
            image[turn, :order] = image_re
            image[turn, order:] = image_im

    right = jnp.concatenate([image_re, image_im], axis=1)
    tall = jnp.concatenate([right, jnp.zeros((128 - order, right.shape[1]), jnp.float32)], axis=0)
    gram = lax.dot_general(
        right, tall, (((1,), (1,)), ((), ())), precision=highest, preferred_element_type=jnp.float32
    )
    part_gram[0] = gram
    land_rep[pl.ds(rep, 1)] = gram[None]
    copies = spread(part_gram.at[0], land_rep.at[rep], send_rep, recv_rep, on_rep, replicas)
    started += copies
    for copy in copies:
        copy.wait_recv()
    gram = land_rep[0]
    for r in range(1, replicas):
        gram = gram + land_rep[r]
    part_gram[1] = gram
    land_grp[pl.ds(grp, 1)] = gram[None]
    copies = spread(part_gram.at[1], land_grp.at[grp], send_grp, recv_grp, on_grp, groups)
    started += copies
    for copy in copies:
        copy.wait_recv()
    gram = land_grp[0]
    for g in range(1, groups):
        gram = gram + land_grp[g]
    gram = gram * (1.0 / (particles * groups * replicas))

    row = lax.broadcasted_iota(jnp.int32, (order, 1), 0)
    for p in range(order):
        pivot = gram[p : p + 1, p : p + 1]
        factor = jnp.where(row > p, gram[:, p : p + 1] / pivot, 0.0)
        scale = jnp.where(row == p, lax.rsqrt(pivot), 1.0)
        right = (right - factor * right[p : p + 1]) * scale
        gram = gram - factor * gram[p : p + 1]
    out_ref[:order] = right[:, :particles]
    out_ref[order:] = right[:, particles:]
    for copy in started:
        copy.wait_send()


def shards(coefficients, truncation, neighbours, initial):
    groups = lax.axis_size("grp")
    replicas = lax.axis_size("rep")
    particles = coefficients.shape[0]
    slots = neighbours.shape[0]
    in_group = neighbours - lax.axis_index("grp") * (replicas * particles)
    padded = jnp.pad(in_group.T, ((0, 0), (0, 128 - slots)))

    mine = coefficients.reshape(particles, 2 * RAD, ANG).transpose(2, 1, 0)
    everyone = lax.all_gather(mine, "rep", axis=0)
    kept = jnp.arange(ANG, dtype=jnp.int32)[:, None] < truncation[None, :]
    kept = jnp.concatenate([kept, kept], axis=1)[:, :, None]
    turned = jnp.concatenate([mine[:, RAD:], -mine[:, :RAD]], axis=1)
    own = jnp.concatenate([mine, turned], axis=2)
    own = jnp.where(kept, own, jnp.zeros_like(own))

    group = replicas * particles
    alignment, operator, degree = pl.pallas_call(
        moments_kernel,
        out_shape=[
            jax.ShapeDtypeStruct((2, slots, particles), jnp.float32),
            jax.ShapeDtypeStruct((group, 2 * particles), jnp.float32),
            jax.ShapeDtypeStruct((1, particles), jnp.float32),
        ],
        in_specs=[VMEM] * 4,
        out_specs=[VMEM] * 3,
        scratch_shapes=[pltpu.VMEM((group, particles), jnp.float32)] * 2,
        name="moments",
    )(own, everyone, in_group, padded)

    rows = initial.shape[0]
    order = rows // 2
    vectors = pl.pallas_call(
        diffuse_kernel,
        out_shape=jax.ShapeDtypeStruct(initial.shape, jnp.float32),
        in_specs=[VMEM] * 3,
        out_specs=VMEM,
        scratch_shapes=[
            pltpu.VMEM((ITERS, replicas, rows, particles), jnp.float32),
            pltpu.VMEM((ITERS - 1, rows, particles), jnp.float32),
            pltpu.VMEM((2, order, 128), jnp.float32),
            pltpu.VMEM((replicas, order, 128), jnp.float32),
            pltpu.VMEM((groups, order, 128), jnp.float32),
            pltpu.SemaphoreType.DMA((ITERS, replicas)),
            pltpu.SemaphoreType.DMA((ITERS, replicas)),
            pltpu.SemaphoreType.DMA((replicas,)),
            pltpu.SemaphoreType.DMA((replicas,)),
            pltpu.SemaphoreType.DMA((groups,)),
            pltpu.SemaphoreType.DMA((groups,)),
        ],
        compiler_params=pltpu.CompilerParams(collective_id=0, has_side_effects=True),
        name="diffuse",
    )(operator, degree, initial)
    return alignment, vectors


def solution(mesh):
    in_specs = (P(("grp", "rep"), None), P(), P(None, ("grp", "rep")), P(None, ("grp", "rep")))
    out_specs = (P(None, None, ("grp", "rep")), P(None, ("grp", "rep")))
    return jax.shard_map(shards, mesh=mesh, in_specs=in_specs, out_specs=out_specs, check_vma=False)
```

```python
import functools
import math

import jax
import jax.numpy as jnp
from jax import lax
from jax.experimental import pallas as pl
from jax.experimental.pallas import tpu as pltpu
from jax.sharding import PartitionSpec as P

ANG = 64
RAD = 16
ITERS = 3
EPS = 1e-06
MESH = pl.DeviceIdType.MESH
VMEM = pl.BlockSpec(memory_space=pltpu.VMEM)


def ring_name(place, across, along):
    column = place // along
    step = place % along
    return (step + (column % 2) * (along - 1 - 2 * step)) * across + column


def ring_place(name, across, along):
    row = name // across
    column = name % across
    return column * along + row + (column % 2) * (along - 1 - 2 * row)


def main_kernel(
    own_ref, mine_ref, slots_ref, initial_ref, ar_ref, ai_ref, out_ref,
    blocks, oper_ref, degree_ref, land, image, part_gram, land_rep, land_grp,
    copy_sem, ring_send, ring_recv, send, recv, send_rep, recv_rep, send_grp, recv_grp,
):
    groups, replicas = lax.axis_size("grp"), lax.axis_size("rep")
    grp, rep = lax.axis_index("grp"), lax.axis_index("rep")
    rows, particles = initial_ref.shape
    order = rows // 2
    highest = lax.Precision.HIGHEST
    own = own_ref.shape[2] // 2
    slots = slots_ref.shape[0]
    half = particles // 2
    along = math.gcd(replicas, 4)
    across = replicas // along
    middle = replicas // 2
    chunk = ANG // 2
    place = ring_place(rep, across, along)
    right_rep = ring_name((place + 1) % replicas, across, along)
    left_rep = ring_name((place + replicas - 1) % replicas, across, along)

    to_first = pltpu.make_async_copy(mine_ref, blocks.at[0], copy_sem)
    to_first.start()

    def on_rep(step):
        return (grp, lax.rem(rep + step, replicas))

    def on_grp(step):
        return (lax.rem(grp + step, groups), rep)

    barrier = pltpu.get_barrier_semaphore()
    for step in range(1, replicas):
        pl.semaphore_signal(barrier, inc=1, device_id=on_rep(step), device_id_type=MESH)
    for step in range(1, groups):
        pl.semaphore_signal(barrier, inc=1, device_id=on_grp(step), device_id_type=MESH)
    pl.semaphore_wait(barrier, replicas + groups - 2)

    def hop(source, slot, part, peer):
        here = pl.ds(part * chunk, chunk)
        return pltpu.make_async_remote_copy(
            src_ref=source.at[here],
            dst_ref=blocks.at[slot, here],
            send_sem=ring_send.at[slot, part],
            recv_sem=ring_recv.at[slot, part],
            device_id=(grp, peer),
            device_id_type=MESH,
        )

    def spread(src, dst, out_sems, in_sems, peer, count):
        copies = []
        for step in range(1, count):
            copy = pltpu.make_async_remote_copy(
                src_ref=src,
                dst_ref=dst,
                send_sem=out_sems.at[step],
                recv_sem=in_sems.at[step],
                device_id=peer(step),
                device_id_type=MESH,
            )
            copy.start()
            copies.append(copy)
        return copies

    first_copies = spread(initial_ref, land.at[0, rep], send.at[0], recv.at[0], on_rep, replicas)
    for part in range(2):
        hop(mine_ref, 1, part, right_rep).start()
        hop(mine_ref, replicas - 1, part, left_rep).start()

    to_first.wait()
    degree_ref[...] = jnp.full(degree_ref.shape, EPS, jnp.float32)

    def block_step(turn, _):
        distance = (turn + 1) // 2
        odd = turn % 2

        @pl.when(jnp.logical_and(odd == 1, distance < middle))
        def _():
            back = replicas - distance
            for part in range(2):
                hop(mine_ref, distance, part, right_rep).wait_recv()

                @pl.when(distance + part < middle)
                def _():
                    hop(blocks.at[distance], distance + 1, part, right_rep).start()

                hop(mine_ref, back, part, left_rep).wait_recv()

                @pl.when(distance + 1 - part < middle)
                def _():
                    hop(blocks.at[back], back - 1, part, left_rep).start()

        @pl.when(jnp.logical_and(odd == 1, distance == middle))
        def _():
            for part in range(2):
                hop(mine_ref, middle, part, right_rep).wait_recv()

        slot = (odd * distance + (1 - odd) * (replicas - distance)) % replicas
        owner = ring_name((place + replicas - slot) % replicas, across, along)

        def tile(part, _):
            energy = moment_re = moment_im = before_re = before_im = None
            for k in range(ANG):
                partner = blocks[slot, k].T
                partner = jnp.where(part == 0, partner[:half], partner[half:])
                spectrum = jnp.dot(partner, own_ref[k], preferred_element_type=jnp.float32)
                re, im = spectrum[:, :own], spectrum[:, own:]
                if k == 0:
                    energy = 2.0 * (re * re)
                    before_re = 2.0 * re
                    continue
                energy = energy + (re * re + im * im)
                if k == 1:
                    moment_re = before_re * re
                    moment_im = -(before_re * im)
                else:
                    moment_re = moment_re + (before_re * re + before_im * im)
                    moment_im = moment_im + (before_im * re - before_re * im)
                before_re, before_im = re, im
            energy, moment_re, moment_im = 0.5 * energy, 0.5 * moment_re, 0.5 * moment_im
            first = pl.multiple_of(owner * particles + part * half, half)
            here = pl.ds(first, half)
            name = lax.broadcasted_iota(jnp.int32, (half, own), 0) + first
            count = jnp.zeros((half, own), jnp.float32)
            for n in range(slots):
                count = count + jnp.where(slots_ref[n : n + 1, :] == name, 1.0, 0.0)
            oper_ref[here, :own] = count * moment_re
            oper_ref[here, own:] = count * moment_im
            degree_ref[...] += jnp.sum(count * energy, axis=0, keepdims=True)
            scale = 1.0 / (energy + EPS)
            ar_ref[here, :] = moment_re * scale
            ai_ref[here, :] = moment_im * scale
            return 0

        lax.fori_loop(0, 2, tile, 0)
        return 0

    lax.fori_loop(0, replicas, block_step, 0)

    started = []
    for turn in range(ITERS):
        src = initial_ref if turn == 0 else image.at[turn - 1]
        if turn == 0:
            copies = first_copies
        else:
            copies = spread(src, land.at[turn, rep], send.at[turn], recv.at[turn], on_rep, replicas)
        land[turn, pl.ds(rep, 1)] = src[...][None]
        started += copies
        for copy in copies:
            copy.wait_recv()
        whole = jnp.concatenate([land[turn, r] for r in range(replicas)], axis=1)
        product = jnp.dot(whole, oper_ref[...], precision=highest, preferred_element_type=jnp.float32)
        image_re = (product[:order, :particles] - product[order:, particles:]) / degree_ref[...]
        image_im = (product[order:, :particles] + product[:order, particles:]) / degree_ref[...]
        if turn < ITERS - 1:
            image[turn, :order] = image_re
            image[turn, order:] = image_im

    right = jnp.concatenate([image_re, image_im], axis=1)
    tall = jnp.concatenate([right, jnp.zeros((128 - order, right.shape[1]), jnp.float32)], axis=0)
    gram = lax.dot_general(
        right, tall, (((1,), (1,)), ((), ())), precision=highest, preferred_element_type=jnp.float32
    )
    part_gram[0] = gram
    land_rep[pl.ds(rep, 1)] = gram[None]
    copies = spread(part_gram.at[0], land_rep.at[rep], send_rep, recv_rep, on_rep, replicas)
    started += copies
    for copy in copies:
        copy.wait_recv()
    gram = land_rep[0]
    for r in range(1, replicas):
        gram = gram + land_rep[r]
    part_gram[1] = gram
    land_grp[pl.ds(grp, 1)] = gram[None]
    copies = spread(part_gram.at[1], land_grp.at[grp], send_grp, recv_grp, on_grp, groups)
    started += copies
    for copy in copies:
        copy.wait_recv()
    gram = land_grp[0]
    for g in range(1, groups):
        gram = gram + land_grp[g]
    gram = gram * (1.0 / (particles * groups * replicas))

    row = lax.broadcasted_iota(jnp.int32, (order, 1), 0)
    for p in range(order):
        pivot = gram[p : p + 1, p : p + 1]
        factor = jnp.where(row > p, gram[:, p : p + 1] / pivot, 0.0)
        scale = jnp.where(row == p, lax.rsqrt(pivot), 1.0)
        right = (right - factor * right[p : p + 1]) * scale
        gram = gram - factor * gram[p : p + 1]
    out_ref[:order] = right[:, :particles]
    out_ref[order:] = right[:, particles:]
    for copy in started:
        copy.wait_send()
    for part in range(2):
        for distance in range(1, replicas):
            if distance != middle:
                hop(mine_ref, distance, part, right_rep).wait_send()
        hop(mine_ref, middle, part, right_rep).wait_send()


def pick_kernel(ar_ref, ai_ref, slots_t_ref, align_ref):
    slots, wide = align_ref.shape[1:]
    names = slots_t_ref[...]
    lane = names % wide
    owner = names // wide

    def pick(block, found):
        rows = pl.ds(pl.multiple_of(block * wide, wide), wide)
        here = owner == block
        got_re = jnp.take_along_axis(ar_ref[rows, :].T, lane, axis=1, mode="promise_in_bounds")
        got_im = jnp.take_along_axis(ai_ref[rows, :].T, lane, axis=1, mode="promise_in_bounds")
        return (jnp.where(here, got_re, found[0]), jnp.where(here, got_im, found[1]))

    zero = jnp.zeros(names.shape, jnp.float32)
    found = lax.fori_loop(0, ar_ref.shape[0] // wide, pick, (zero, zero))
    align_ref[0] = found[0].T[:slots]
    align_ref[1] = found[1].T[:slots]


def shards(coefficients, truncation, neighbours, initial):
    groups = lax.axis_size("grp")
    replicas = lax.axis_size("rep")
    particles = coefficients.shape[0]
    slots = neighbours.shape[0]
    in_group = neighbours - lax.axis_index("grp") * (replicas * particles)
    padded = jnp.pad(in_group.T, ((0, 0), (0, 128 - slots)))

    mine = coefficients.reshape(particles, 2 * RAD, ANG).transpose(2, 1, 0)
    kept = jnp.arange(ANG, dtype=jnp.int32)[:, None] < truncation[None, :]
    kept = jnp.concatenate([kept, kept], axis=1)[:, :, None]
    turned = jnp.concatenate([mine[:, RAD:], -mine[:, :RAD]], axis=1)
    own = jnp.concatenate([mine, turned], axis=2)
    own = jnp.where(kept, own, jnp.zeros_like(own))

    group = replicas * particles
    rows = initial.shape[0]
    order = rows // 2
    dma = pltpu.SemaphoreType.DMA
    table = jax.ShapeDtypeStruct((group, particles), jnp.float32)
    ratio_re, ratio_im, vectors = pl.pallas_call(
        main_kernel,
        out_shape=[table, table, jax.ShapeDtypeStruct(initial.shape, jnp.float32)],
        in_specs=[VMEM] * 4,
        out_specs=[VMEM] * 3,
        scratch_shapes=[
            pltpu.VMEM((replicas,) + mine.shape, mine.dtype),
            pltpu.VMEM((group, 2 * particles), jnp.float32),
            pltpu.VMEM((1, particles), jnp.float32),
            pltpu.VMEM((ITERS, replicas, rows, particles), jnp.float32),
            pltpu.VMEM((ITERS - 1, rows, particles), jnp.float32),
            pltpu.VMEM((2, order, 128), jnp.float32),
            pltpu.VMEM((replicas, order, 128), jnp.float32),
            pltpu.VMEM((groups, order, 128), jnp.float32),
            dma,
            dma((replicas, 2)),
            dma((replicas, 2)),
            dma((ITERS, replicas)),
            dma((ITERS, replicas)),
            dma((replicas,)),
            dma((replicas,)),
            dma((groups,)),
            dma((groups,)),
        ],
        compiler_params=pltpu.CompilerParams(collective_id=0, has_side_effects=True),
        name="main",
    )(own, mine, in_group, initial)
    alignment = pl.pallas_call(
        pick_kernel,
        out_shape=jax.ShapeDtypeStruct((2, slots, particles), jnp.float32),
        in_specs=[VMEM] * 3,
        out_specs=VMEM,
        name="pick",
    )(ratio_re, ratio_im, padded)
    return alignment, vectors


def solution(mesh):
    in_specs = (P(("grp", "rep"), None), P(), P(None, ("grp", "rep")), P(None, ("grp", "rep")))
    out_specs = (P(None, None, ("grp", "rep")), P(None, ("grp", "rep")))
    return jax.shard_map(shards, mesh=mesh, in_specs=in_specs, out_specs=out_specs, check_vma=False)
```

```python
import functools
import math

import jax
import jax.numpy as jnp
from jax import lax
from jax.experimental import pallas as pl
from jax.experimental.pallas import tpu as pltpu
from jax.sharding import PartitionSpec as P

ANG = 64
RAD = 16
ITERS = 3
EPS = 1e-06
MESH = pl.DeviceIdType.MESH
VMEM = pl.BlockSpec(memory_space=pltpu.VMEM)


def ring_name(place, across, along):
    column = place // along
    step = place % along
    return (step + (column % 2) * (along - 1 - 2 * step)) * across + column


def ring_place(name, across, along):
    row = name // across
    column = name % across
    return column * along + row + (column % 2) * (along - 1 - 2 * row)


def main_kernel(
    own_ref, mine_ref, slots_ref, slots_t_ref, initial_ref, align_ref, out_ref,
    ratio, found, blocks, oper_ref, degree_ref, land, image, part_gram, land_rep, land_grp,
    copy_sem, ring_send, ring_recv, send, recv, send_rep, recv_rep, send_grp, recv_grp,
):
    groups, replicas = lax.axis_size("grp"), lax.axis_size("rep")
    grp, rep = lax.axis_index("grp"), lax.axis_index("rep")
    rows, particles = initial_ref.shape
    order = rows // 2
    highest = lax.Precision.HIGHEST
    own = own_ref.shape[2] // 2
    slots = slots_ref.shape[0]
    half = particles // 2
    along = math.gcd(replicas, 4)
    across = replicas // along
    middle = replicas // 2
    chunk = ANG // 2
    place = ring_place(rep, across, along)
    right_rep = ring_name((place + 1) % replicas, across, along)
    left_rep = ring_name((place + replicas - 1) % replicas, across, along)

    to_first = pltpu.make_async_copy(mine_ref, blocks.at[0], copy_sem)
    to_first.start()

    def on_rep(step):
        return (grp, lax.rem(rep + step, replicas))

    def on_grp(step):
        return (lax.rem(grp + step, groups), rep)

    barrier = pltpu.get_barrier_semaphore()
    for step in range(1, replicas):
        pl.semaphore_signal(barrier, inc=1, device_id=on_rep(step), device_id_type=MESH)
    for step in range(1, groups):
        pl.semaphore_signal(barrier, inc=1, device_id=on_grp(step), device_id_type=MESH)
    pl.semaphore_wait(barrier, replicas + groups - 2)

    def hop(source, slot, part, peer):
        here = pl.ds(part * chunk, chunk)
        return pltpu.make_async_remote_copy(
            src_ref=source.at[here],
            dst_ref=blocks.at[slot, here],
            send_sem=ring_send.at[slot, part],
            recv_sem=ring_recv.at[slot, part],
            device_id=(grp, peer),
            device_id_type=MESH,
        )

    def spread(src, dst, out_sems, in_sems, peer, count):
        copies = []
        for step in range(1, count):
            copy = pltpu.make_async_remote_copy(
                src_ref=src,
                dst_ref=dst,
                send_sem=out_sems.at[step],
                recv_sem=in_sems.at[step],
                device_id=peer(step),
                device_id_type=MESH,
            )
            copy.start()
            copies.append(copy)
        return copies

    first_copies = spread(initial_ref, land.at[0, rep], send.at[0], recv.at[0], on_rep, replicas)
    for part in range(2):
        hop(mine_ref, 1, part, right_rep).start()
        hop(mine_ref, replicas - 1, part, left_rep).start()

    to_first.wait()
    found[...] = jnp.zeros_like(found)
    degree_ref[...] = jnp.full(degree_ref.shape, EPS, jnp.float32)

    def block_step(turn, _):
        distance = (turn + 1) // 2
        odd = turn % 2

        @pl.when(jnp.logical_and(odd == 1, distance < middle))
        def _():
            back = replicas - distance
            for part in range(2):
                hop(mine_ref, distance, part, right_rep).wait_recv()

                @pl.when(distance + part < middle)
                def _():
                    hop(blocks.at[distance], distance + 1, part, right_rep).start()

                hop(mine_ref, back, part, left_rep).wait_recv()

                @pl.when(distance + 1 - part < middle)
                def _():
                    hop(blocks.at[back], back - 1, part, left_rep).start()

        @pl.when(jnp.logical_and(odd == 1, distance == middle))
        def _():
            for part in range(2):
                hop(mine_ref, middle, part, right_rep).wait_recv()

        slot = (odd * distance + (1 - odd) * (replicas - distance)) % replicas
        owner = ring_name((place + replicas - slot) % replicas, across, along)

        def tile(part, _):
            energy = moment_re = moment_im = before_re = before_im = None
            for k in range(ANG):
                partner = blocks[slot, k].T
                partner = jnp.where(part == 0, partner[:half], partner[half:])
                spectrum = jnp.dot(partner, own_ref[k], preferred_element_type=jnp.float32)
                re, im = spectrum[:, :own], spectrum[:, own:]
                if k == 0:
                    energy = 2.0 * (re * re)
                    before_re = 2.0 * re
                    continue
                energy = energy + (re * re + im * im)
                if k == 1:
                    moment_re = before_re * re
                    moment_im = -(before_re * im)
                else:
                    moment_re = moment_re + (before_re * re + before_im * im)
                    moment_im = moment_im + (before_im * re - before_re * im)
                before_re, before_im = re, im
            energy, moment_re, moment_im = 0.5 * energy, 0.5 * moment_re, 0.5 * moment_im
            first = pl.multiple_of(owner * particles + part * half, half)
            here = pl.ds(first, half)
            name = lax.broadcasted_iota(jnp.int32, (half, own), 0) + first
            count = jnp.zeros((half, own), jnp.float32)
            for n in range(slots):
                count = count + jnp.where(slots_ref[n : n + 1, :] == name, 1.0, 0.0)
            oper_ref[here, :own] = count * moment_re
            oper_ref[here, own:] = count * moment_im
            degree_ref[...] += jnp.sum(count * energy, axis=0, keepdims=True)
            scale = 1.0 / (energy + EPS)
            local = pl.ds(pl.multiple_of(part * half, half), half)
            ratio[0, local] = moment_re * scale
            ratio[1, local] = moment_im * scale
            return 0

        lax.fori_loop(0, 2, tile, 0)
        names = slots_t_ref[...]
        here = names // particles == owner
        lane = names % particles
        for side in range(2):
            got = jnp.take_along_axis(ratio[side].T, lane, axis=1, mode="promise_in_bounds")
            found[side] = jnp.where(here, got, found[side])
        return 0

    lax.fori_loop(0, replicas, block_step, 0)
    for side in range(2):
        align_ref[side] = found[side].T[:slots]

    started = []
    for turn in range(ITERS):
        src = initial_ref if turn == 0 else image.at[turn - 1]
        if turn == 0:
            copies = first_copies
        else:
            copies = spread(src, land.at[turn, rep], send.at[turn], recv.at[turn], on_rep, replicas)
        land[turn, pl.ds(rep, 1)] = src[...][None]
        started += copies
        for copy in copies:
            copy.wait_recv()
        whole = jnp.concatenate([land[turn, r] for r in range(replicas)], axis=1)
        product = jnp.dot(whole, oper_ref[...], precision=highest, preferred_element_type=jnp.float32)
        image_re = (product[:order, :particles] - product[order:, particles:]) / degree_ref[...]
        image_im = (product[order:, :particles] + product[:order, particles:]) / degree_ref[...]
        if turn < ITERS - 1:
            image[turn, :order] = image_re
            image[turn, order:] = image_im

    right = jnp.concatenate([image_re, image_im], axis=1)
    tall = jnp.concatenate([right, jnp.zeros((128 - order, right.shape[1]), jnp.float32)], axis=0)
    gram = lax.dot_general(
        right, tall, (((1,), (1,)), ((), ())), precision=highest, preferred_element_type=jnp.float32
    )
    part_gram[0] = gram
    land_rep[pl.ds(rep, 1)] = gram[None]
    copies = spread(part_gram.at[0], land_rep.at[rep], send_rep, recv_rep, on_rep, replicas)
    started += copies
    for copy in copies:
        copy.wait_recv()
    gram = land_rep[0]
    for r in range(1, replicas):
        gram = gram + land_rep[r]
    part_gram[1] = gram
    land_grp[pl.ds(grp, 1)] = gram[None]
    copies = spread(part_gram.at[1], land_grp.at[grp], send_grp, recv_grp, on_grp, groups)
    started += copies
    for copy in copies:
        copy.wait_recv()
    gram = land_grp[0]
    for g in range(1, groups):
        gram = gram + land_grp[g]
    gram = gram * (1.0 / (particles * groups * replicas))

    row = lax.broadcasted_iota(jnp.int32, (order, 1), 0)
    for p in range(order):
        pivot = gram[p : p + 1, p : p + 1]
        factor = jnp.where(row > p, gram[:, p : p + 1] / pivot, 0.0)
        scale = jnp.where(row == p, lax.rsqrt(pivot), 1.0)
        right = (right - factor * right[p : p + 1]) * scale
        gram = gram - factor * gram[p : p + 1]
    out_ref[:order] = right[:, :particles]
    out_ref[order:] = right[:, particles:]
    for copy in started:
        copy.wait_send()
    for part in range(2):
        for distance in range(1, replicas):
            if distance != middle:
                hop(mine_ref, distance, part, right_rep).wait_send()
        hop(mine_ref, middle, part, right_rep).wait_send()


def shards(coefficients, truncation, neighbours, initial):
    groups = lax.axis_size("grp")
    replicas = lax.axis_size("rep")
    particles = coefficients.shape[0]
    slots = neighbours.shape[0]
    in_group = neighbours - lax.axis_index("grp") * (replicas * particles)
    padded = jnp.pad(in_group.T, ((0, 0), (0, 128 - slots)))

    mine = coefficients.reshape(particles, 2 * RAD, ANG).transpose(2, 1, 0)
    kept = jnp.arange(ANG, dtype=jnp.int32)[:, None] < truncation[None, :]
    kept = jnp.concatenate([kept, kept], axis=1)[:, :, None]
    turned = jnp.concatenate([mine[:, RAD:], -mine[:, :RAD]], axis=1)
    own = jnp.concatenate([mine, turned], axis=2)
    own = jnp.where(kept, own, jnp.zeros_like(own))

    group = replicas * particles
    rows = initial.shape[0]
    order = rows // 2
    dma = pltpu.SemaphoreType.DMA
    alignment, vectors = pl.pallas_call(
        main_kernel,
        out_shape=[
            jax.ShapeDtypeStruct((2, slots, particles), jnp.float32),
            jax.ShapeDtypeStruct(initial.shape, jnp.float32),
        ],
        in_specs=[VMEM] * 5,
        out_specs=[VMEM] * 2,
        scratch_shapes=[
            pltpu.VMEM((2, particles, particles), jnp.float32),
            pltpu.VMEM((2,) + padded.shape, jnp.float32),
            pltpu.VMEM((replicas,) + mine.shape, mine.dtype),
            pltpu.VMEM((group, 2 * particles), jnp.float32),
            pltpu.VMEM((1, particles), jnp.float32),
            pltpu.VMEM((ITERS, replicas, rows, particles), jnp.float32),
            pltpu.VMEM((ITERS - 1, rows, particles), jnp.float32),
            pltpu.VMEM((2, order, 128), jnp.float32),
            pltpu.VMEM((replicas, order, 128), jnp.float32),
            pltpu.VMEM((groups, order, 128), jnp.float32),
            dma,
            dma((replicas, 2)),
            dma((replicas, 2)),
            dma((ITERS, replicas)),
            dma((ITERS, replicas)),
            dma((replicas,)),
            dma((replicas,)),
            dma((groups,)),
            dma((groups,)),
        ],
        compiler_params=pltpu.CompilerParams(collective_id=0, has_side_effects=True),
        name="main",
    )(own, mine, in_group, padded, initial)
    return alignment, vectors


def solution(mesh):
    in_specs = (P(("grp", "rep"), None), P(), P(None, ("grp", "rep")), P(None, ("grp", "rep")))
    out_specs = (P(None, None, ("grp", "rep")), P(None, ("grp", "rep")))
    return jax.shard_map(shards, mesh=mesh, in_specs=in_specs, out_specs=out_specs, check_vma=False)
```
